256 devices in a mesh: groups: 4 (over x, y), patch: 64 (over z, core).
Axes of the slice: x: 2, y: 2, z: 32, core: 2. Of those that a mesh axis runs over, the one named last changes fastest.
The devices are a block of a 4x8x32 slice.
Arguments:
- tokens: bfloat16 [131072, 1152], P(('groups', 'patch')), parts along dimension 0, may hold values from -6 to 6
- stale_kv: bfloat16 [131072, 1152], P(('groups', 'patch')), parts along dimension 0, may hold values from -40 to 40, as said below
- mod_table: float32 [6, 1152], replicated, may hold values from -2 to 3
- mod_mix: float32 [6, 1152], replicated, may hold values from -3 to 3
- timestep: int32 [4], P('groups'), parts along dimension 0, may hold values from 0 to 999
- frame_order: int32 [64], P('groups'), parts along dimension 0, may hold values from 0 to 15, each once
- spatial_qkv: bfloat16 [3, 1152, 576], replicated, may hold values from -0.1875 to 0.1875
- spatial_out: bfloat16 [576, 1152], replicated, may hold values from -0.25 to 0.25
- temporal_qkv: bfloat16 [3, 1152, 576], replicated, may hold values from -0.1875 to 0.1875
- temporal_out: bfloat16 [576, 1152], replicated, may hold values from -0.25 to 0.25
Outputs:
- block_out: float32 [131072, 1152], P(('groups', 'patch')), parts along dimension 0
The draws below stay inside these ranges and needn't reach their ends.
There are 4 independent parts, one for each index of `groups`. The reference program is written for one: setup_inputs(seed, part) draws one part's arguments, and reference() takes and returns one part's arrays. A program takes and returns all parts, laid end to end along the dimension named above; an argument that names none is the same for every part. Nothing has to cross between parts.
Inputs may be any that keep to these rules, and one draw needn't show every extreme that they name: `frame_order`: a permutation of the 16 time positions. `stale_kv`: previous step's keys and values.
All inputs are finite; a program needn't handle non-finite values.
Results may differ from the reference program's by a relative error of at most 0.013.
The reference program's roundings to bfloat16 on the way count: a program that leaves them out, or rounds other values in their place, can miss the bound.
Values may be sent and summed in bfloat16 or wider, within the bound.
A program may use at most 128 MiB of HBM per device.

```python
import math
import jax
import jax.numpy as jnp
from jax import lax

D = 1152
HEADS = 16
HEADS_WIN = 8
WIN = 576
PATCH_TOK = 512
FRAMES = 16
FRAME_TOK = 2048
TOKENS = 32768


def draw_stale_kv(key, part):
    width_win = HEADS_WIN * (D // HEADS)
    base = jnp.clip(jax.random.normal(jax.random.fold_in(key, 11), (TOKENS, 2 * width_win), jnp.float32), -5.0, 5.0)
    return base.astype(jnp.bfloat16)


def draw_mod_table(key, part):
    table = jnp.clip(0.5 * jax.random.normal(jax.random.fold_in(key, 21), (6, D), jnp.float32), -2.0, 2.0)
    return table


def levels(rng, shape, split, smallest, largest):
    loudness, own = 1.0, jax.random.fold_in(rng, 6)
    for axis_at, blocks in split:
        heights = jnp.exp(jax.random.uniform(jax.random.fold_in(own, axis_at), (blocks,), jnp.float32, smallest / len(split), largest / len(split)))
        loudness = loudness * jnp.repeat(heights, shape[axis_at] // blocks).reshape([-1 if axis == axis_at else 1 for axis in range(len(shape))])
    return loudness


def scatter_about(own_key, shape, width, limit, shards=(), kind=jnp.bfloat16):
    entries = jax.random.normal(own_key, shape, jnp.float32) * width
    if len(shards) > 0:
        entries = levels(own_key, shape, shards, -0.22, 0.18) * entries
    return jnp.clip(entries, min=-limit, max=limit).astype(kind)


def setup_inputs(seed: int = 0, part: int = 0) -> dict:
    key_list = jax.random.split(jax.random.key(seed), 11)
    part_keys = jax.random.split(jax.random.fold_in(key_list[10], part), 11)
    tokens = scatter_about(part_keys[0], (TOKENS, D), 1.0, 6.0, ((0, 64),))
    stale_kv = draw_stale_kv(jax.random.fold_in(jax.random.fold_in(key_list[10], part), 71), part)
    mod_table = draw_mod_table(jax.random.fold_in(key_list[10], 71), part)
    mod_mix = scatter_about(key_list[3], (6, D), 0.5, 3.0, (), jnp.float32)
    timestep = jax.random.randint(part_keys[4], (1,), 0, 1000).astype(jnp.int32)
    frame_order = jax.random.permutation(part_keys[5], FRAMES).astype(jnp.int32)
    spatial_qkv = scatter_about(key_list[6], (3, D, WIN), D ** -0.5, 0.1875)
    spatial_out = scatter_about(key_list[7], (WIN, D), WIN ** -0.5, 0.25)
    temporal_qkv = scatter_about(key_list[8], (3, D, WIN), D ** -0.5, 0.1875)
    temporal_out = scatter_about(key_list[9], (WIN, D), WIN ** -0.5, 0.25)
    return {"tokens": tokens, "stale_kv": stale_kv, "mod_table": mod_table, "mod_mix": mod_mix, "timestep": timestep, "frame_order": frame_order, "spatial_qkv": spatial_qkv, "spatial_out": spatial_out, "temporal_qkv": temporal_qkv, "temporal_out": temporal_out}


epsilon = 1e-06

def normalize(activations):
    row_mean = lax.optimization_barrier(jnp.mean(activations, axis=-1, keepdims=True))
    centered = activations - row_mean
    variance = lax.optimization_barrier(jnp.mean(centered * centered, axis=-1, keepdims=True))
    return centered * lax.rsqrt(variance + epsilon)

def sinusoid(position, feature_width):
    half_width = feature_width // 2
    frequencies = jnp.exp(-math.log(10000.0) * jnp.arange(half_width, dtype=jnp.float32) / half_width)
    angles = jnp.asarray(position).astype(jnp.float32)[..., None] * frequencies
    return jnp.concatenate([jnp.sin(angles), jnp.cos(angles)], axis=-1)

def softmax_rows(scores):
    row_top = lax.optimization_barrier(jnp.max(scores, axis=-1, keepdims=True))
    exp_scores = jnp.exp(scores - row_top)
    return (exp_scores / lax.optimization_barrier(jnp.sum(exp_scores, axis=-1, keepdims=True))).astype(jnp.bfloat16)

def project(inputs, weight):
    return jnp.dot(inputs, weight, preferred_element_type=jnp.float32)

def spatial_attend(queries, key_rows, value_rows):
    head_dim = D // HEADS
    query_heads = queries.reshape(-1, HEADS_WIN, head_dim).astype(jnp.float32)
    key_heads = key_rows.reshape(-1, HEADS_WIN, head_dim).astype(jnp.float32)
    value_heads = value_rows.reshape(-1, HEADS_WIN, head_dim).astype(jnp.float32)
    scores = jnp.einsum('qhe,khe->hqk', query_heads, key_heads) * head_dim ** (-0.5)
    weights = softmax_rows(scores)
    mixed_out = jnp.einsum('hqk,khe->qhe', weights.astype(jnp.float32), value_heads)
    return mixed_out.reshape(-1, HEADS_WIN * head_dim).astype(jnp.bfloat16)

def temporal_attend(queries, key_rows, value_rows):
    head_dim = D // HEADS
    frame_count = queries.shape[0]
    pixel_count = queries.shape[1]
    shape_heads = (frame_count, pixel_count, HEADS_WIN, head_dim)
    query_heads = queries.reshape(shape_heads).astype(jnp.float32)
    key_heads = key_rows.reshape(shape_heads).astype(jnp.float32)
    value_heads = value_rows.reshape(shape_heads).astype(jnp.float32)
    scores = jnp.einsum('fmhe,gmhe->mhfg', query_heads, key_heads) * head_dim ** (-0.5)
    weights = softmax_rows(scores)
    mixed_out = jnp.einsum('mhfg,gmhe->fmhe', weights.astype(jnp.float32), value_heads)
    return mixed_out.reshape(frame_count, pixel_count, HEADS_WIN * head_dim).astype(jnp.bfloat16)

def reference(tokens, stale_kv, mod_table, mod_mix, timestep, frame_order, spatial_qkv, spatial_out, temporal_qkv, temporal_out):
    width_win = HEADS_WIN * (D // HEADS)
    modulation = mod_table + mod_mix * sinusoid(timestep[0], D)[None, :]
    tokens_wide = tokens.astype(jnp.float32)
    spatial_in = (normalize(tokens_wide) * (1.0 + modulation[1]) + modulation[0]).astype(jnp.bfloat16)
    quartered = (FRAMES, 4, PATCH_TOK, width_win)
    fresh_q = project(spatial_in, spatial_qkv[0]).astype(jnp.bfloat16).reshape(quartered)
    fresh_k = project(spatial_in, spatial_qkv[1]).astype(jnp.bfloat16).reshape(quartered)
    fresh_v = project(spatial_in, spatial_qkv[2]).astype(jnp.bfloat16).reshape(quartered)
    stale_k = stale_kv[:, :width_win].reshape(quartered)
    stale_v = stale_kv[:, width_win:].reshape(quartered)

    def one_frame(inputs):
        frame_q, frame_k, frame_v, old_k, old_v = inputs
        results = []
        for quarter in range(4):
            key_rows = jnp.concatenate([frame_k[source] if source == quarter else old_k[source] for source in range(4)], axis=0)
            value_rows = jnp.concatenate([frame_v[source] if source == quarter else old_v[source] for source in range(4)], axis=0)
            results.append(spatial_attend(frame_q[quarter], key_rows, value_rows))
        return jnp.stack(results)
    spatial_mixed = lax.map(one_frame, (fresh_q, fresh_k, fresh_v, stale_k, stale_v)).reshape(TOKENS, width_win)
    after_spatial = tokens_wide + modulation[2] * project(spatial_mixed, spatial_out)
    positions = sinusoid(frame_order, D)
    temporal_in = normalize(after_spatial).reshape(FRAMES, FRAME_TOK, D) * (1.0 + modulation[4]) + modulation[3] + positions[:, None, :]
    temporal_in = temporal_in.astype(jnp.bfloat16).reshape(TOKENS, D)
    framed = (FRAMES, FRAME_TOK, width_win)
    temporal_q = project(temporal_in, temporal_qkv[0]).astype(jnp.bfloat16).reshape(framed)
    temporal_k = project(temporal_in, temporal_qkv[1]).astype(jnp.bfloat16).reshape(framed)
    temporal_v = project(temporal_in, temporal_qkv[2]).astype(jnp.bfloat16).reshape(framed)
    temporal_mixed = temporal_attend(temporal_q, temporal_k, temporal_v).reshape(TOKENS, width_win)
    return after_spatial + modulation[5] * project(temporal_mixed, temporal_out)
```

```python
import functools
import math

import jax
import jax.numpy as jnp
from jax import lax
from jax.experimental import pallas as pl
from jax.experimental.pallas import tpu as pltpu
from jax.sharding import PartitionSpec as P

HEADS = 16
EPS = 1e-06
MESH = pl.DeviceIdType.MESH
F32 = jnp.float32
BF16 = jnp.bfloat16
LANES = 128
WINDOW = 256
TURNS = 2
KV_ROWS = (0, 256, 512)
NEG = -1e30


def sinusoid(position, feature_width):
    half_width = feature_width // 2
    frequencies = jnp.exp(
        -math.log(10000.0) * jnp.arange(half_width, dtype=F32) / half_width
    )
    angles = jnp.asarray(position).astype(F32)[..., None] * frequencies
    return jnp.concatenate([jnp.sin(angles), jnp.cos(angles)], axis=-1)


def normalize(v):
    inverse = 1.0 / v.shape[-1]
    mean = jnp.sum(v, axis=-1, keepdims=True) * inverse
    centered = v - mean
    variance = jnp.sum(centered * centered, axis=-1, keepdims=True) * inverse
    return centered * lax.rsqrt(variance + EPS)


def dot(a, b):
    return jnp.dot(a, b, preferred_element_type=F32)


def dot_t(a, b):
    return lax.dot_general(a, b, (((1,), (1,)), ((), ())), preferred_element_type=F32)


def window_start(column, most):
    return pl.multiple_of(jnp.minimum(column // LANES, most) * LANES, LANES)


def wide(x, width):
    return jnp.concatenate([x] * (width // LANES), axis=1) if width > LANES else x


def kernel(
    tokens, stale, mods, wqkv, wout, tqkv, tout, out,
    tok, kvb, wq, wo, tw, two, xin, qb, qm, mx, sm, acc, mixed, after, xs, xr,
    tq, tk, tv, tmix, osend, orecv, obuf,
    load_sem, kv_send, kv_recv, part_recv, fwd_recv, x_send, x_recv, o_send, o_recv, out_sem,
):
    rows, width = tok.shape
    win = wout.shape[0]
    head_dim = width // HEADS
    heads = win // head_dim
    devices = lax.axis_size("patch")
    frames = devices // 4
    piece = rows // frames // TURNS
    chunk = rows // (2 * TURNS)
    scale = head_dim ** (-0.5) * math.log2(math.e)
    me = lax.axis_index("patch")
    frame, quarter = me // 4, me % 4
    partner = frame * 4 + quarter + 1 - 2 * (quarter % 2)
    across = quarter + 2 - 4 * (quarter // 2)
    opposite = frame * 4 + across
    kv_most = width // LANES - WINDOW // LANES
    q_most = qb.shape[1] // LANES - WINDOW // LANES
    v_tile0 = win // LANES
    pad = win - v_tile0 * LANES

    def remote(src, dst, send, recv, device):
        return pltpu.make_async_remote_copy(
            src_ref=src, dst_ref=dst, send_sem=send, recv_sem=recv,
            device_id={"patch": device}, device_id_type=MESH,
        )

    loads = [
        (tokens, tok), (wqkv, wq), (wout, wo.at[pl.ds(pad, win), :]), (tqkv, tw), (tout, two),
    ]
    loads = [pltpu.make_async_copy(a, b, load_sem.at[i]) for i, (a, b) in enumerate(loads)]
    for copy in loads:
        copy.start()

    barrier = pltpu.get_barrier_semaphore()
    pl.semaphore_signal(barrier, inc=1, device_id={"patch": partner}, device_id_type=MESH)

    def greet(j, c):
        pl.semaphore_signal(
            barrier, inc=1, device_id={"patch": j * 4 + across}, device_id_type=MESH
        )
        return c

    lax.fori_loop(0, frames, greet, 0)
    pl.semaphore_wait(barrier, frames + 1)

    kv_pieces = list(zip(KV_ROWS[:-1], KV_ROWS[1:]))
    for n, (lo, hi) in enumerate(kv_pieces):
        part = stale.at[pl.ds(lo, hi - lo), :]
        remote(part, kvb.at[2, pl.ds(lo, hi - lo), :], kv_send.at[0], kv_recv.at[n], opposite).start()
    remote(stale, kvb.at[1], kv_send.at[1], part_recv, partner).start()

    wo[pl.ds(0, pad), :] = jnp.zeros((pad, width), BF16)
    for ref in (qb, tq, tk, tv):
        ref[...] = jnp.zeros(ref.shape, ref.dtype)
    mixed[...] = jnp.zeros(mixed.shape, mixed.dtype)

    shift_s, scale_s, gate_s = mods[0:1, :], mods[1:2, :], mods[2:3, :]
    shift_t, scale_t, gate_t = mods[3:4, :], mods[4:5, :], mods[5:6, :]

    loads[0].wait()

    def fresh_in(i, c):
        at = pl.ds(pl.multiple_of(i * chunk, chunk), chunk)
        v = normalize(tok[at, :].astype(F32))
        xin[at, :] = (v * scale_s + shift_s).astype(BF16)
        return c

    lax.fori_loop(0, rows // chunk, fresh_in, 0)
    loads[1].wait()

    def fresh(i, c):
        at = pl.ds(pl.multiple_of(i * WINDOW, WINDOW), WINDOW)
        x = xin[at, :]
        qb[at, 0:win] = dot_t(x, wq[0]).astype(BF16)
        kvb[0, at, 0:win] = dot_t(x, wq[1]).astype(BF16)
        kvb[0, at, win : 2 * win] = dot_t(x, wq[2]).astype(BF16)
        return c

    lax.fori_loop(0, rows // WINDOW, fresh, 0)

    def of_head(start, column, count):
        lane = lax.broadcasted_iota(jnp.int32, (count, WINDOW), 1) + start
        return (lane >= column) & (lane < column + head_dim)

    def mask_q(h, c):
        start = window_start(h * head_dim, q_most)
        q = qb[:, pl.ds(start, WINDOW)]
        qm[h] = jnp.where(of_head(start, h * head_dim, rows), q, jnp.zeros_like(q))
        mx[h] = jnp.full((rows, LANES), NEG, F32)
        sm[h] = jnp.zeros((rows, LANES), F32)
        acc[h] = jnp.zeros((rows, WINDOW), F32)
        return c

    lax.fori_loop(0, heads, mask_q, 0)

    def attend(h, blocks):
        k_at = window_start(h * head_dim, q_most)
        v_at = window_start(win + h * head_dim, kv_most)
        q = qm[h]
        scores = [dot_t(q, kvb[s, at, pl.ds(k_at, WINDOW)]) for s, at in blocks]
        top = jnp.max(scores[0], axis=-1, keepdims=True)
        for s in scores[1:]:
            top = jnp.maximum(top, jnp.max(s, axis=-1, keepdims=True))
        old = mx[h]
        new = jnp.maximum(old, top)
        mx[h] = new
        fade = jnp.exp2((old - new) * scale)
        total = 0.0
        product = 0.0
        for (s, at), score in zip(blocks, scores):
            e = jnp.exp2((score - wide(new, score.shape[1])) * scale)
            total = total + jnp.sum(e, axis=-1, keepdims=True)
            product = product + dot(e.astype(BF16), kvb[s, at, pl.ds(v_at, WINDOW)])
        sm[h] = sm[h] * fade + total
        acc[h] = acc[h] * wide(fade, WINDOW) + product

    whole = pl.ds(0, rows)
    lax.fori_loop(0, heads, lambda h, c: (attend(h, [(0, whole)]), c)[1], 0)
    remote(stale, kvb.at[1], kv_send.at[1], part_recv, partner).wait_recv()
    lax.fori_loop(0, heads, lambda h, c: (attend(h, [(1, whole)]), c)[1], 0)

    for n, (lo, hi) in enumerate(kv_pieces):
        at = pl.ds(lo, hi - lo)
        remote(stale.at[at, :], kvb.at[2, at, :], kv_send.at[0], kv_recv.at[n], opposite).wait_recv()
        forward = remote(
            kvb.at[2, at, :], kvb.at[3, at, :], kv_send.at[2], fwd_recv.at[n], partner
        )
        forward.start()
        forward.wait_recv()
        lax.fori_loop(0, heads, lambda h, c: (attend(h, [(2, at), (3, at)]), c)[1], 0)

    loads[2].wait()

    def finish(u, c):
        at = pl.ds(pl.multiple_of(u * chunk, chunk), chunk)

        def place(h, c):
            v_at = window_start(win + h * head_dim, kv_most)
            m_at = pl.ds(pl.multiple_of(v_at - v_tile0 * LANES, LANES), WINDOW)
            value = (acc[h, at, :] / wide(sm[h, at, :], WINDOW)).astype(BF16)
            keep = of_head(v_at, win + h * head_dim, chunk)
            mixed[at, m_at] = jnp.where(keep, value, mixed[at, m_at])
            return c

        lax.fori_loop(0, heads, place, 0)
        done = tok[at, :].astype(F32) + gate_s * dot(mixed[at, :], wo[...])
        after[at, :] = done
        xs[at, :] = (normalize(done) * scale_t + shift_t).astype(BF16)
        turn = u // 2
        for i in (3, 4, 2, 5, 1, 6, 0, 7):
            m = 2 * i + (u + frame) % 2
            j = (frame + m) % frames
            src = pl.ds(pl.multiple_of(u * chunk + (j // 2) * piece, piece), piece)
            remote(
                xs.at[src, :], xr.at[turn, frame], x_send, x_recv.at[turn], j * 4 + across
            ).start()
        return c

    lax.fori_loop(0, 2 * TURNS, finish, 0)

    loads[3].wait()
    block = frames * piece
    same = (
        lax.broadcasted_iota(jnp.int32, (block, block), 0) % piece
        == lax.broadcasted_iota(jnp.int32, (block, block), 1) % piece
    )

    def temporal(turn, c):
        remote(xr.at[turn], xr.at[turn], x_send, x_recv.at[turn], opposite).wait_recv()
        x = xr[turn].reshape(block, width)
        tq[:, 0:win] = dot_t(x, tw[0]).astype(BF16)
        tk[:, 0:win] = dot_t(x, tw[1]).astype(BF16)
        tv[:, 0:win] = dot_t(x, tw[2]).astype(BF16)

        def one_head(h, c):
            start = window_start(h * head_dim, q_most)
            at = pl.ds(start, WINDOW)
            keep = of_head(start, h * head_dim, block)
            q = tq[:, at]
            score = dot_t(jnp.where(keep, q, jnp.zeros_like(q)), tk[:, at])
            score = jnp.where(same, score, NEG)
            top = jnp.max(score, axis=-1, keepdims=True)
            e = jnp.where(same, jnp.exp2((score - top) * scale), 0.0)
            weights = (e / jnp.sum(e, axis=-1, keepdims=True)).astype(BF16)
            value = dot(weights, tv[:, at]).astype(BF16)
            tmix[:, at] = jnp.where(keep, value, tmix[:, at])
            return c

        lax.fori_loop(0, heads, one_head, 0)
        osend[turn] = tmix[:, 0:win].reshape(frames, piece, win)
        row = turn * (rows // TURNS) + (frame % 2) * chunk + (frame // 2) * piece
        row = pl.multiple_of(row, piece)
        for i in (7, 8, 6, 9, 5, 10, 4, 11, 3, 12, 2, 13, 1, 14, 0, 15):
            j = (frame + i) % frames
            remote(
                osend.at[turn, j], orecv.at[pl.ds(row, piece), :], o_send, o_recv.at[turn],
                j * 4 + across,
            ).start()
        return c

    tmix[...] = jnp.zeros(tmix.shape, tmix.dtype)
    lax.fori_loop(0, TURNS, temporal, 0)

    loads[4].wait()
    half = rows // TURNS

    def last(turn, c):
        at = pl.ds(pl.multiple_of(turn * half, half), half)
        remote(orecv.at[at, :], orecv.at[at, :], o_send, o_recv.at[turn], opposite).wait_recv()
        obuf[at, :] = after[at, :] + gate_t * dot(orecv[at, :], two[...])
        pltpu.make_async_copy(obuf.at[at, :], out.at[at, :], out_sem).start()
        return c

    lax.fori_loop(0, TURNS, last, 0)
    pltpu.make_async_copy(obuf, out, out_sem).wait()
    remote(stale, kvb.at[2], kv_send.at[0], kv_recv.at[0], opposite).wait_send()
    remote(stale, kvb.at[1], kv_send.at[1], part_recv, partner).wait_send()
    remote(kvb.at[2], kvb.at[3], kv_send.at[2], fwd_recv.at[0], partner).wait_send()
    remote(xs, xs, x_send, x_recv.at[0], opposite).wait_send()
    remote(osend, osend, o_send, o_recv.at[0], opposite).wait_send()


def per_device(
    tokens, stale_kv, mod_table, mod_mix, timestep, frame_order,
    spatial_qkv, spatial_out, temporal_qkv, temporal_out,
):
    rows, width = tokens.shape
    win = spatial_out.shape[0]
    heads = win // (width // HEADS)
    frames = lax.axis_size("patch") // 4
    piece = rows // frames // TURNS
    frame = lax.axis_index("patch") // 4
    modulation = mod_table + mod_mix * sinusoid(timestep[0], width)[None, :]
    frame_id = jnp.sum(jnp.where(jnp.arange(frames) == frame, frame_order, 0))
    emb = sinusoid(frame_id, width)
    row_id = jnp.arange(8)[:, None]
    mods = jnp.concatenate([modulation, modulation[:2]], axis=0)
    mods = mods + jnp.where((row_id == 1) | (row_id == 4), 1.0, 0.0)
    mods = mods + jnp.where(row_id == 3, emb[None, :], 0.0)
    padded = -(-win // LANES) * LANES
    block = frames * piece
    any_spec = pl.BlockSpec(memory_space=pl.ANY)
    pieces = len(KV_ROWS) - 1
    dma = pltpu.SemaphoreType.DMA
    return pl.pallas_call(
        kernel,
        out_shape=jax.ShapeDtypeStruct((rows, width), F32),
        in_specs=[any_spec, any_spec, pl.BlockSpec(memory_space=pltpu.VMEM)] + [any_spec] * 4,
        out_specs=any_spec,
        scratch_shapes=[
            pltpu.VMEM((rows, width), BF16),
            pltpu.VMEM((4, rows, width), BF16),
            pltpu.VMEM((3, win, width), BF16),
            pltpu.VMEM((padded, width), BF16),
            pltpu.VMEM((3, win, width), BF16),
            pltpu.VMEM((win, width), BF16),
            pltpu.VMEM((rows, width), BF16),
            pltpu.VMEM((rows, padded), BF16),
            pltpu.VMEM((heads, rows, WINDOW), BF16),
            pltpu.VMEM((heads, rows, LANES), F32),
            pltpu.VMEM((heads, rows, LANES), F32),
            pltpu.VMEM((heads, rows, WINDOW), F32),
            pltpu.VMEM((rows, padded), BF16),
            pltpu.VMEM((rows, width), F32),
            pltpu.VMEM((rows, width), BF16),
            pltpu.VMEM((TURNS, frames, piece, width), BF16),
            pltpu.VMEM((block, padded), BF16),
            pltpu.VMEM((block, padded), BF16),
            pltpu.VMEM((block, padded), BF16),
            pltpu.VMEM((block, padded), BF16),
            pltpu.VMEM((TURNS, frames, piece, win), BF16),
            pltpu.VMEM((rows, win), BF16),
            pltpu.VMEM((rows, width), F32),
            dma((5,)), dma((3,)), dma((pieces,)), dma, dma((pieces,)),
            dma, dma((TURNS,)), dma, dma((TURNS,)), dma,
        ],
        compiler_params=pltpu.CompilerParams(
            collective_id=0, has_side_effects=True, vmem_limit_bytes=60 * 1024 * 1024
        ),
        name="block",
    )(
        tokens, stale_kv, mods, jnp.swapaxes(spatial_qkv, 1, 2), spatial_out,
        jnp.swapaxes(temporal_qkv, 1, 2), temporal_out,
    )


def solution(mesh):
    return jax.shard_map(
        per_device,
        mesh=mesh,
        in_specs=(
            P(("groups", "patch"), None), P(("groups", "patch"), None), P(), P(),
            P("groups"), P("groups"), P(), P(), P(), P(),
        ),
        out_specs=P(("groups", "patch"), None),
        check_vma=False,
    )
```

```python
import functools
import math

import jax
import jax.numpy as jnp
from jax import lax
from jax.experimental import pallas as pl
from jax.experimental.pallas import tpu as pltpu
from jax.sharding import PartitionSpec as P

HEADS = 16
EPS = 1e-06
MESH = pl.DeviceIdType.MESH
F32 = jnp.float32
BF16 = jnp.bfloat16
LANES = 128
WINDOW = 256
UNROLL = 8
TURNS = 2
KV_ROWS = (0, 256, 384, 512)
NEG = -1e30


def sinusoid(position, feature_width):
    half_width = feature_width // 2
    frequencies = jnp.exp(
        -math.log(10000.0) * jnp.arange(half_width, dtype=F32) / half_width
    )
    angles = jnp.asarray(position).astype(F32)[..., None] * frequencies
    return jnp.concatenate([jnp.sin(angles), jnp.cos(angles)], axis=-1)


def normalize(v):
    inverse = 1.0 / v.shape[-1]
    mean = jnp.sum(v, axis=-1, keepdims=True) * inverse
    centered = v - mean
    variance = jnp.sum(centered * centered, axis=-1, keepdims=True) * inverse
    return centered * lax.rsqrt(variance + EPS)


def dot(a, b):
    return jnp.dot(a, b, preferred_element_type=F32)


def dot_t(a, b):
    return lax.dot_general(a, b, (((1,), (1,)), ((), ())), preferred_element_type=F32)


def window_start(column, most):
    return pl.multiple_of(jnp.minimum(column // LANES, most) * LANES, LANES)


def wide(x, width):
    return jnp.concatenate([x] * (width // LANES), axis=1) if width > LANES else x


def kernel(
    tokens, stale, mods, wqkv, wout, tqkv, tout, out,
    tok, kvb, wq, wo, tw, two, xin, qb, qm, mx, sm, acc, mixed, after, xs, xr,
    tq, tk, tv, tmix, osend, orecv,
    load_sem, kv_send, kv_recv, part_recv, fwd_recv, x_send, x_recv, o_send, o_recv, known,
):
    rows, width = tok.shape
    win = wout.shape[0]
    head_dim = width // HEADS
    heads = win // head_dim
    devices = lax.axis_size("patch")
    frames = devices // 4
    piece = rows // frames // TURNS
    chunk = rows // (2 * TURNS)
    scale = head_dim ** (-0.5) * math.log2(math.e)
    me = lax.axis_index("patch")
    frame, quarter = me // 4, me % 4
    partner = frame * 4 + quarter + 1 - 2 * (quarter % 2)
    across = quarter + 2 - 4 * (quarter // 2)
    opposite = frame * 4 + across
    kv_most = width // LANES - WINDOW // LANES
    q_most = qb.shape[1] // LANES - WINDOW // LANES
    v_tile0 = win // LANES
    pad = win - v_tile0 * LANES

    def remote(src, dst, send, recv, device):
        return pltpu.make_async_remote_copy(
            src_ref=src, dst_ref=dst, send_sem=send, recv_sem=recv,
            device_id={"patch": device}, device_id_type=MESH,
        )

    loads = [
        (tokens, tok), (wqkv, wq), (wout, wo.at[pl.ds(pad, win), :]), (tqkv, tw), (tout, two.at[pl.ds(0, win), :]),
    ]
    loads = [pltpu.make_async_copy(a, b, load_sem.at[i]) for i, (a, b) in enumerate(loads)]
    for copy in loads:
        copy.start()

    barrier = pltpu.get_barrier_semaphore()
    before, after_me = (frame + frames - 1) % frames, (frame + 1) % frames
    near = [partner, opposite]
    for j in (before, after_me):
        near += [j * 4 + quarter, j * 4 + across]
    for device in near:
        pl.semaphore_signal(barrier, inc=1, device_id={"patch": device}, device_id_type=MESH)
    pl.semaphore_wait(barrier, len(near))

    distances = [1 << n for n in range(frames.bit_length() - 2)]

    def say(n):
        for away in (distances[n], frames - distances[n]):
            j = (frame + away) % frames
            pl.semaphore_signal(
                known.at[n], inc=1, device_id={"patch": j * 4 + quarter}, device_id_type=MESH
            )

    def hear(n):
        pl.semaphore_wait(known.at[n], 2)

    kv_pieces = list(zip(KV_ROWS[:-1], KV_ROWS[1:]))
    for n, (lo, hi) in enumerate(kv_pieces):
        part = stale.at[pl.ds(lo, hi - lo), :]
        remote(part, kvb.at[2, pl.ds(lo, hi - lo), :], kv_send.at[0], kv_recv.at[n], opposite).start()
    remote(stale, kvb.at[1], kv_send.at[1], part_recv, partner).start()

    say(0)

    wo[pl.ds(0, pad), :] = jnp.zeros((pad, width), BF16)
    two[pl.ds(win, two.shape[0] - win), :] = jnp.zeros((two.shape[0] - win, width), BF16)
    for ref in (qb, tq, tk, tv):
        ref[...] = jnp.zeros(ref.shape, ref.dtype)
    mixed[...] = jnp.zeros(mixed.shape, mixed.dtype)

    shift_s, scale_s, gate_s = mods[0:1, :], mods[1:2, :], mods[2:3, :]
    shift_t, scale_t, gate_t = mods[3:4, :], mods[4:5, :], mods[5:6, :]

    loads[0].wait()

    def fresh_in(i, c):
        at = pl.ds(pl.multiple_of(i * chunk, chunk), chunk)
        v = normalize(tok[at, :].astype(F32))
        xin[at, :] = (v * scale_s + shift_s).astype(BF16)
        return c

    lax.fori_loop(0, rows // chunk, fresh_in, 0)
    hear(0)
    say(1)
    loads[1].wait()

    def fresh(i, c):
        at = pl.ds(pl.multiple_of(i * WINDOW, WINDOW), WINDOW)
        x = xin[at, :]
        qb[at, 0:win] = dot_t(x, wq[0]).astype(BF16)
        kvb[0, at, 0:win] = dot_t(x, wq[1]).astype(BF16)
        kvb[0, at, win : 2 * win] = dot_t(x, wq[2]).astype(BF16)
        return c

    lax.fori_loop(0, rows // WINDOW, fresh, 0)
    for n in range(1, len(distances) - 1):
        hear(n)
        say(n + 1)

    whole = pl.ds(0, rows)

    def of_head(start, column, count):
        lane = lax.broadcasted_iota(jnp.int32, (count, WINDOW), 1) + start
        return (lane >= column) & (lane < column + head_dim)

    def each_head(step):
        lax.fori_loop(0, heads, lambda h, c: (step(h), c)[1], 0, unroll=UNROLL)

    def mask_q(h, c):
        start = window_start(h * head_dim, q_most)
        q = qb[:, pl.ds(start, WINDOW)]
        qm[h] = jnp.where(of_head(start, h * head_dim, rows), q, jnp.zeros_like(q))
        mx[h] = jnp.full((rows, LANES), NEG, F32)
        sm[h] = jnp.zeros((rows, LANES), F32)
        acc[h] = jnp.zeros((rows, WINDOW), F32)
        return c

    lax.fori_loop(0, heads, mask_q, 0)

    def attend(h, blocks, own=whole):
        k_at = window_start(h * head_dim, q_most)
        v_at = window_start(win + h * head_dim, kv_most)
        q = qm[h, own, :]
        scores = [dot_t(q, kvb[s, at, pl.ds(k_at, WINDOW)]) for s, at in blocks]
        top = jnp.max(scores[0], axis=-1, keepdims=True)
        for s in scores[1:]:
            top = jnp.maximum(top, jnp.max(s, axis=-1, keepdims=True))
        old = mx[h, own, :]
        new = jnp.maximum(old, top)
        mx[h, own, :] = new
        fade = jnp.exp2((old - new) * scale)
        total = 0.0
        product = 0.0
        for (s, at), score in zip(blocks, scores):
            e = jnp.exp2((score - wide(new, score.shape[1])) * scale)
            total = total + jnp.sum(e, axis=-1, keepdims=True)
            product = product + dot(e.astype(BF16), kvb[s, at, pl.ds(v_at, WINDOW)])
        sm[h, own, :] = sm[h, own, :] * fade + total
        acc[h, own, :] = acc[h, own, :] * wide(fade, WINDOW) + product

    each_head(lambda h: attend(h, [(0, whole)]))
    remote(stale, kvb.at[1], kv_send.at[1], part_recv, partner).wait_recv()
    each_head(lambda h: attend(h, [(1, whole)]))

    for n, (lo, hi) in enumerate(kv_pieces):
        at = pl.ds(lo, hi - lo)
        remote(stale.at[at, :], kvb.at[2, at, :], kv_send.at[0], kv_recv.at[n], opposite).wait_recv()
        forward = remote(
            kvb.at[2, at, :], kvb.at[3, at, :], kv_send.at[2], fwd_recv.at[n], partner
        )
        forward.start()
        forward.wait_recv()
        if hi < rows:
            each_head(lambda h: attend(h, [(2, at), (3, at)]))

    loads[2].wait()

    for n in range(max(len(distances) - 1, 0), len(distances)):
        hear(n)
    final = pl.ds(kv_pieces[-1][0], rows - kv_pieces[-1][0])

    def finish(u, c):
        at = pl.ds(pl.multiple_of(u * chunk, chunk), chunk)
        each_head(lambda h: attend(h, [(2, final), (3, final)], at))

        def place(h):
            v_at = window_start(win + h * head_dim, kv_most)
            m_at = pl.ds(pl.multiple_of(v_at - v_tile0 * LANES, LANES), WINDOW)
            value = (acc[h, at, :] / wide(sm[h, at, :], WINDOW)).astype(BF16)
            keep = of_head(v_at, win + h * head_dim, chunk)
            mixed[at, m_at] = jnp.where(keep, value, mixed[at, m_at])

        each_head(place)
        done = tok[at, :].astype(F32) + gate_s * dot(mixed[at, :], wo[...])
        after[at, :] = done
        xs[at, :] = (normalize(done) * scale_t + shift_t).astype(BF16)
        turn = u // 2
        for i in (3, 4, 2, 5, 1, 6, 0, 7):
            m = 2 * i + (u + frame) % 2
            j = (frame + m) % frames
            src = pl.ds(pl.multiple_of(u * chunk + (j // 2) * piece, piece), piece)
            remote(
                xs.at[src, :], xr.at[turn, frame], x_send, x_recv.at[turn], j * 4 + across
            ).start()
        return c

    lax.fori_loop(0, 2 * TURNS, finish, 0)

    loads[3].wait()
    full = win // LANES
    block = frames * piece
    same = (
        lax.broadcasted_iota(jnp.int32, (block, block), 0) % piece
        == lax.broadcasted_iota(jnp.int32, (block, block), 1) % piece
    )

    def temporal(turn, c):
        remote(xr.at[turn], xr.at[turn], x_send, x_recv.at[turn], opposite).wait_recv()
        x = xr[turn].reshape(block, width)
        tq[:, 0:win] = dot_t(x, tw[0]).astype(BF16)
        tk[:, 0:win] = dot_t(x, tw[1]).astype(BF16)
        tv[:, 0:win] = dot_t(x, tw[2]).astype(BF16)

        def one_head(h):
            start = window_start(h * head_dim, q_most)
            at = pl.ds(start, WINDOW)
            keep = of_head(start, h * head_dim, block)
            q = tq[:, at]
            score = dot_t(jnp.where(keep, q, jnp.zeros_like(q)), tk[:, at])
            score = jnp.where(same, score, NEG)
            top = jnp.max(score, axis=-1, keepdims=True)
            e = jnp.where(same, jnp.exp2((score - top) * scale), 0.0)
            weights = (e / jnp.sum(e, axis=-1, keepdims=True)).astype(BF16)
            value = dot(weights, tv[:, at]).astype(BF16)
            tmix[:, at] = jnp.where(keep, value, tmix[:, at])

        each_head(one_head)
        for n in range(full):
            part = tmix[:, n * LANES : (n + 1) * LANES]
            osend[turn, :, n * piece : (n + 1) * piece, :] = part.reshape(frames, piece, LANES)
        tail = tmix[:, full * LANES : (full + 1) * LANES].astype(F32)
        tail = tail.reshape(frames, 2, piece // 2, LANES)
        tail = tail[:, 0] + pltpu.roll(tail[:, 1].reshape(block // 2, LANES), LANES // 2, 1).reshape(
            frames, piece // 2, LANES
        )
        osend[turn, :, full * piece :, :] = tail.astype(BF16)
        slot = (frame % 2) * (frames // 2) + frame // 2
        for i in (7, 8, 6, 9, 5, 10, 4, 11, 3, 12, 2, 13, 1, 14, 0, 15):
            j = (frame + i) % frames
            remote(
                osend.at[turn, j], orecv.at[turn, slot], o_send, o_recv.at[turn],
                j * 4 + across,
            ).start()
        return c

    tmix[...] = jnp.zeros(tmix.shape, tmix.dtype)
    lax.fori_loop(0, TURNS, temporal, 0)

    loads[4].wait()
    half = rows // TURNS

    def last(turn, c):
        at = pl.ds(pl.multiple_of(turn * half, half), half)
        remote(orecv.at[turn], orecv.at[turn], o_send, o_recv.at[turn], opposite).wait_recv()
        parts = [
            orecv[turn, :, n * piece : (n + 1) * piece, :].reshape(half, LANES)
            for n in range(full)
        ]
        tail = orecv[turn, :, full * piece :, :].astype(F32)
        low = pltpu.roll(tail.reshape(half // 2, LANES), LANES // 2, 1)
        tail = jnp.concatenate([tail, low.reshape(tail.shape)], axis=1)
        parts.append(tail.reshape(half, LANES).astype(BF16))
        out[at, :] = after[at, :] + gate_t * dot(jnp.concatenate(parts, axis=1), two[...])
        return c

    lax.fori_loop(0, TURNS, last, 0)
    remote(stale, kvb.at[2], kv_send.at[0], kv_recv.at[0], opposite).wait_send()
    remote(stale, kvb.at[1], kv_send.at[1], part_recv, partner).wait_send()
    remote(kvb.at[2], kvb.at[3], kv_send.at[2], fwd_recv.at[0], partner).wait_send()
    remote(xs, xs, x_send, x_recv.at[0], opposite).wait_send()
    remote(osend, osend, o_send, o_recv.at[0], opposite).wait_send()


def per_device(
    tokens, stale_kv, mod_table, mod_mix, timestep, frame_order,
    spatial_qkv, spatial_out, temporal_qkv, temporal_out,
):
    rows, width = tokens.shape
    win = spatial_out.shape[0]
    heads = win // (width // HEADS)
    frames = lax.axis_size("patch") // 4
    piece = rows // frames // TURNS
    frame = lax.axis_index("patch") // 4
    modulation = mod_table + mod_mix * sinusoid(timestep[0], width)[None, :]
    frame_id = jnp.sum(jnp.where(jnp.arange(frames) == frame, frame_order, 0))
    emb = sinusoid(frame_id, width)
    row_id = jnp.arange(8)[:, None]
    mods = jnp.concatenate([modulation, modulation[:2]], axis=0)
    mods = mods + jnp.where((row_id == 1) | (row_id == 4), 1.0, 0.0)
    mods = mods + jnp.where(row_id == 3, emb[None, :], 0.0)
    padded = -(-win // LANES) * LANES
    block = frames * piece
    any_spec = pl.BlockSpec(memory_space=pl.ANY)
    pieces = len(KV_ROWS) - 1
    dma = pltpu.SemaphoreType.DMA
    return pl.pallas_call(
        kernel,
        out_shape=pltpu.VMEM((rows, width), F32),
        in_specs=[any_spec, any_spec, pl.BlockSpec(memory_space=pltpu.VMEM)] + [any_spec] * 4,
        out_specs=pl.BlockSpec(memory_space=pltpu.VMEM),
        scratch_shapes=[
            pltpu.VMEM((rows, width), BF16),
            pltpu.VMEM((4, rows, width), BF16),
            pltpu.VMEM((3, win, width), BF16),
            pltpu.VMEM((padded, width), BF16),
            pltpu.VMEM((3, win, width), BF16),
            pltpu.VMEM((padded, width), BF16),
            pltpu.VMEM((rows, width), BF16),
            pltpu.VMEM((rows, padded), BF16),
            pltpu.VMEM((heads, rows, WINDOW), BF16),
            pltpu.VMEM((heads, rows, LANES), F32),
            pltpu.VMEM((heads, rows, LANES), F32),
            pltpu.VMEM((heads, rows, WINDOW), F32),
            pltpu.VMEM((rows, padded), BF16),
            pltpu.VMEM((rows, width), F32),
            pltpu.VMEM((rows, width), BF16),
            pltpu.VMEM((TURNS, frames, piece, width), BF16),
            pltpu.VMEM((block, padded), BF16),
            pltpu.VMEM((block, padded), BF16),
            pltpu.VMEM((block, padded), BF16),
            pltpu.VMEM((block, padded), BF16),
            pltpu.VMEM((TURNS, frames, piece * win // LANES, LANES), BF16),
            pltpu.VMEM((TURNS, frames, piece * win // LANES, LANES), BF16),
            dma((5,)), dma((3,)), dma((pieces,)), dma, dma((pieces,)),
            dma, dma((TURNS,)), dma, dma((TURNS,)),
            pltpu.SemaphoreType.REGULAR((max(frames.bit_length() - 2, 1),)),
        ],
        compiler_params=pltpu.CompilerParams(
            collective_id=0, has_side_effects=True, vmem_limit_bytes=52 * 1024 * 1024
        ),
        name="block",
    )(
        tokens, stale_kv, mods, jnp.swapaxes(spatial_qkv, 1, 2), spatial_out,
        jnp.swapaxes(temporal_qkv, 1, 2), temporal_out,
    )


def solution(mesh):
    return jax.shard_map(
        per_device,
        mesh=mesh,
        in_specs=(
            P(("groups", "patch"), None), P(("groups", "patch"), None), P(), P(),
            P("groups"), P("groups"), P(), P(), P(), P(),
        ),
        out_specs=P(("groups", "patch"), None),
        check_vma=False,
    )
```

```python
import functools
import math

import jax
import jax.numpy as jnp
import numpy as np
from jax import lax
from jax.experimental import pallas as pl
from jax.experimental.pallas import tpu as pltpu
from jax.sharding import PartitionSpec as P

HEADS = 16
EPS = 1e-06
MESH = pl.DeviceIdType.MESH
F32 = jnp.float32
BF16 = jnp.bfloat16
LANES = 128
WINDOW = 256
UNROLL = 8
TURNS = 2
KV_ROWS = (0, 256, 384, 512)
NEG = -1e30


def angular_rates(feature_width):
    half_width = feature_width // 2
    rates = np.exp(-math.log(10000.0) * np.arange(half_width, dtype=np.float64) / half_width)
    return np.concatenate([rates, rates]).astype(np.float32)[None, :]


def sinusoid(position, rates):
    width = rates.shape[1]
    upper = lax.broadcasted_iota(jnp.int32, (1, width), 1) >= width // 2
    angle = position.astype(F32) * rates
    turn = jnp.floor(angle * (2.0 / math.pi) + 0.5)
    x = angle - turn * 1.5703125
    x = x - turn * 4.837512969970703125e-4
    x = x - turn * 7.54978995489188216e-8
    z = x * x
    sine = ((-1.9515295891e-4 * z + 8.3321608736e-3) * z - 1.6666654611e-1) * z * x + x
    cosine = (2.443315711809948e-5 * z - 1.388731625493765e-3) * z + 4.166664568298827e-2
    cosine = cosine * z * z - 0.5 * z + 1.0
    quarter = turn + jnp.where(upper, 1.0, 0.0)
    quarter = quarter - 4.0 * jnp.floor(quarter * 0.25)
    odd = (quarter == 1.0) | (quarter == 3.0)
    value = jnp.where(odd, cosine, sine)
    return jnp.where(quarter >= 2.0, -value, value)


def normalize(v):
    inverse = 1.0 / v.shape[-1]
    mean = jnp.sum(v, axis=-1, keepdims=True) * inverse
    centered = v - mean
    variance = jnp.sum(centered * centered, axis=-1, keepdims=True) * inverse
    return centered * lax.rsqrt(variance + EPS)


def dot(a, b):
    return jnp.dot(a, b, preferred_element_type=F32)


def dot_t(a, b):
    return lax.dot_general(a, b, (((1,), (1,)), ((), ())), preferred_element_type=F32)


def window_start(column, most):
    return pl.multiple_of(jnp.minimum(column // LANES, most) * LANES, LANES)


def wide(x, width):
    return jnp.concatenate([x] * (width // LANES), axis=1) if width > LANES else x


def kernel(
    tokens, stale, table_in, mix_in, time_in, order_in, rates_in, wqkv, wout, tqkv, tout, out,
    table, mix, time, order, rates, mods,
    tok, kvb, wq, wo, tw, two, xin, qb, qm, mx, sm, acc, mixed, after, xs, xr,
    tq, tk, tv, tmix, osend, orecv,
    small_sem, load_sem, kv_send, kv_recv, part_recv, fwd_recv, x_send, x_recv, o_send, o_recv, known,
):
    rows, width = tok.shape
    win = wout.shape[0]
    head_dim = width // HEADS
    heads = win // head_dim
    devices = lax.axis_size("patch")
    frames = devices // 4
    piece = rows // frames // TURNS
    chunk = rows // (2 * TURNS)
    scale = head_dim ** (-0.5) * math.log2(math.e)
    me = lax.axis_index("patch")
    frame, quarter = me // 4, me % 4
    partner = frame * 4 + quarter + 1 - 2 * (quarter % 2)
    across = quarter + 2 - 4 * (quarter // 2)
    opposite = frame * 4 + across
    kv_most = width // LANES - WINDOW // LANES
    q_most = qb.shape[1] // LANES - WINDOW // LANES
    v_tile0 = win // LANES
    pad = win - v_tile0 * LANES

    def remote(src, dst, send, recv, device):
        return pltpu.make_async_remote_copy(
            src_ref=src, dst_ref=dst, send_sem=send, recv_sem=recv,
            device_id={"patch": device}, device_id_type=MESH,
        )

    barrier = pltpu.get_barrier_semaphore()
    before, after_me = (frame + frames - 1) % frames, (frame + 1) % frames
    near = [partner, opposite]
    for j in (before, after_me):
        near += [j * 4 + quarter, j * 4 + across]
    for device in near:
        pl.semaphore_signal(barrier, inc=1, device_id={"patch": device}, device_id_type=MESH)

    loads = [
        (tokens, tok), (wqkv, wq), (wout, wo.at[pl.ds(pad, win), :]), (tqkv, tw), (tout, two.at[pl.ds(0, win), :]),
    ]
    small = [
        (table_in, table), (mix_in, mix), (time_in, time), (order_in, order), (rates_in, rates),
    ]
    small = [pltpu.make_async_copy(a, b, small_sem.at[i]) for i, (a, b) in enumerate(small)]
    loads = [pltpu.make_async_copy(a, b, load_sem.at[i]) for i, (a, b) in enumerate(loads)]
    for copy in loads[:1] + small + loads[1:]:
        copy.start()
    pl.semaphore_wait(barrier, len(near))

    distances = [1 << n for n in range(frames.bit_length() - 2)]

    def say(n):
        for away in (distances[n], frames - distances[n]):
            j = (frame + away) % frames
            pl.semaphore_signal(
                known.at[n], inc=1, device_id={"patch": j * 4 + quarter}, device_id_type=MESH
            )

    def hear(n):
        pl.semaphore_wait(known.at[n], 2)

    kv_pieces = list(zip(KV_ROWS[:-1], KV_ROWS[1:]))
    for n, (lo, hi) in enumerate(kv_pieces):
        part = stale.at[pl.ds(lo, hi - lo), :]
        remote(part, kvb.at[2, pl.ds(lo, hi - lo), :], kv_send.at[0], kv_recv.at[n], opposite).start()
    remote(stale, kvb.at[1], kv_send.at[1], part_recv, partner).start()

    say(0)

    wo[pl.ds(0, pad), :] = jnp.zeros((pad, width), BF16)
    two[pl.ds(win, two.shape[0] - win), :] = jnp.zeros((two.shape[0] - win, width), BF16)
    for ref in (qb, tq, tk, tv):
        ref[...] = jnp.zeros(ref.shape, ref.dtype)
    mixed[...] = jnp.zeros(mixed.shape, mixed.dtype)

    for copy in small:
        copy.wait()
    mods[...] = table[...] + mix[...] * sinusoid(time[0], rates[...])
    position = sinusoid(order[frame], rates[...])
    shift_s, scale_s, gate_s = mods[0:1, :], 1.0 + mods[1:2, :], mods[2:3, :]
    shift_t, scale_t, gate_t = mods[3:4, :] + position, 1.0 + mods[4:5, :], mods[5:6, :]

    loads[0].wait()

    def fresh_in(i, c):
        at = pl.ds(pl.multiple_of(i * chunk, chunk), chunk)
        v = normalize(tok[at, :].astype(F32))
        xin[at, :] = (v * scale_s + shift_s).astype(BF16)
        return c

    lax.fori_loop(0, rows // chunk, fresh_in, 0)
    hear(0)
    say(1)
    loads[1].wait()

    def fresh(i, c):
        at = pl.ds(pl.multiple_of(i * WINDOW, WINDOW), WINDOW)
        x = xin[at, :]
        qb[at, 0:win] = dot_t(x, wq[0]).astype(BF16)
        kvb[0, at, 0:win] = dot_t(x, wq[1]).astype(BF16)
        kvb[0, at, win : 2 * win] = dot_t(x, wq[2]).astype(BF16)
        return c

    lax.fori_loop(0, rows // WINDOW, fresh, 0)
    for n in range(1, len(distances) - 1):
        hear(n)
        say(n + 1)

    whole = pl.ds(0, rows)

    def of_head(start, column, count):
        lane = lax.broadcasted_iota(jnp.int32, (count, WINDOW), 1) + start
        return (lane >= column) & (lane < column + head_dim)

    def each_head(step):
        lax.fori_loop(0, heads, lambda h, c: (step(h), c)[1], 0, unroll=UNROLL)

    def mask_q(h, c):
        start = window_start(h * head_dim, q_most)
        q = qb[:, pl.ds(start, WINDOW)]
        qm[h] = jnp.where(of_head(start, h * head_dim, rows), q, jnp.zeros_like(q))
        mx[h] = jnp.full((rows, LANES), NEG, F32)
        sm[h] = jnp.zeros((rows, LANES), F32)
        acc[h] = jnp.zeros((rows, WINDOW), F32)
        return c

    lax.fori_loop(0, heads, mask_q, 0)

    def attend(h, blocks, own=whole):
        k_at = window_start(h * head_dim, q_most)
        v_at = window_start(win + h * head_dim, kv_most)
        q = qm[h, own, :]
        scores = [dot_t(q, kvb[s, at, pl.ds(k_at, WINDOW)]) for s, at in blocks]
        top = jnp.max(scores[0], axis=-1, keepdims=True)
        for s in scores[1:]:
            top = jnp.maximum(top, jnp.max(s, axis=-1, keepdims=True))
        old = mx[h, own, :]
        new = jnp.maximum(old, top)
        mx[h, own, :] = new
        fade = jnp.exp2((old - new) * scale)
        total = 0.0
        product = 0.0
        for (s, at), score in zip(blocks, scores):
            e = jnp.exp2((score - wide(new, score.shape[1])) * scale)
            total = total + jnp.sum(e, axis=-1, keepdims=True)
            product = product + dot(e.astype(BF16), kvb[s, at, pl.ds(v_at, WINDOW)])
        sm[h, own, :] = sm[h, own, :] * fade + total
        acc[h, own, :] = acc[h, own, :] * wide(fade, WINDOW) + product

    each_head(lambda h: attend(h, [(0, whole)]))
    remote(stale, kvb.at[1], kv_send.at[1], part_recv, partner).wait_recv()
    each_head(lambda h: attend(h, [(1, whole)]))

    for n, (lo, hi) in enumerate(kv_pieces):
        at = pl.ds(lo, hi - lo)
        remote(stale.at[at, :], kvb.at[2, at, :], kv_send.at[0], kv_recv.at[n], opposite).wait_recv()
        forward = remote(
            kvb.at[2, at, :], kvb.at[3, at, :], kv_send.at[2], fwd_recv.at[n], partner
        )
        forward.start()
        forward.wait_recv()
        if hi < rows:
            each_head(lambda h: attend(h, [(2, at), (3, at)]))

    loads[2].wait()

    for n in range(max(len(distances) - 1, 0), len(distances)):
        hear(n)
    final = pl.ds(kv_pieces[-1][0], rows - kv_pieces[-1][0])

    def finish(u, c):
        at = pl.ds(pl.multiple_of(u * chunk, chunk), chunk)
        each_head(lambda h: attend(h, [(2, final), (3, final)], at))

        def place(h):
            v_at = window_start(win + h * head_dim, kv_most)
            m_at = pl.ds(pl.multiple_of(v_at - v_tile0 * LANES, LANES), WINDOW)
            value = (acc[h, at, :] / wide(sm[h, at, :], WINDOW)).astype(BF16)
            keep = of_head(v_at, win + h * head_dim, chunk)
            mixed[at, m_at] = jnp.where(keep, value, mixed[at, m_at])

        each_head(place)
        done = tok[at, :].astype(F32) + gate_s * dot(mixed[at, :], wo[...])
        after[at, :] = done
        xs[at, :] = (normalize(done) * scale_t + shift_t).astype(BF16)
        turn = u // 2
        for i in (3, 4, 2, 5, 1, 6, 0, 7):
            m = 2 * i + (u + frame) % 2
            j = (frame + m) % frames
            src = pl.ds(pl.multiple_of(u * chunk + (j // 2) * piece, piece), piece)
            remote(
                xs.at[src, :], xr.at[turn, frame], x_send, x_recv.at[turn], j * 4 + across
            ).start()
        return c

    lax.fori_loop(0, 2 * TURNS, finish, 0)

    loads[3].wait()
    full = win // LANES
    block = frames * piece
    same = (
        lax.broadcasted_iota(jnp.int32, (block, block), 0) % piece
        == lax.broadcasted_iota(jnp.int32, (block, block), 1) % piece
    )

    def temporal(turn, c):
        remote(xr.at[turn], xr.at[turn], x_send, x_recv.at[turn], opposite).wait_recv()
        x = xr[turn].reshape(block, width)
        tq[:, 0:win] = dot_t(x, tw[0]).astype(BF16)
        tk[:, 0:win] = dot_t(x, tw[1]).astype(BF16)
        tv[:, 0:win] = dot_t(x, tw[2]).astype(BF16)

        def one_head(h):
            start = window_start(h * head_dim, q_most)
            at = pl.ds(start, WINDOW)
            keep = of_head(start, h * head_dim, block)
            q = tq[:, at]
            score = dot_t(jnp.where(keep, q, jnp.zeros_like(q)), tk[:, at])
            score = jnp.where(same, score, NEG)
            top = jnp.max(score, axis=-1, keepdims=True)
            e = jnp.where(same, jnp.exp2((score - top) * scale), 0.0)
            weights = (e / jnp.sum(e, axis=-1, keepdims=True)).astype(BF16)
            value = dot(weights, tv[:, at]).astype(BF16)
            tmix[:, at] = jnp.where(keep, value, tmix[:, at])

        each_head(one_head)
        for n in range(full):
            part = tmix[:, n * LANES : (n + 1) * LANES]
            osend[turn, :, n * piece : (n + 1) * piece, :] = part.reshape(frames, piece, LANES)
        tail = tmix[:, full * LANES : (full + 1) * LANES].astype(F32)
        tail = tail.reshape(frames, 2, piece // 2, LANES)
        tail = tail[:, 0] + pltpu.roll(tail[:, 1].reshape(block // 2, LANES), LANES // 2, 1).reshape(
            frames, piece // 2, LANES
        )
        osend[turn, :, full * piece :, :] = tail.astype(BF16)
        slot = (frame % 2) * (frames // 2) + frame // 2
        for i in (7, 8, 6, 9, 5, 10, 4, 11, 3, 12, 2, 13, 1, 14, 0, 15):
            j = (frame + i) % frames
            remote(
                osend.at[turn, j], orecv.at[turn, slot], o_send, o_recv.at[turn],
                j * 4 + across,
            ).start()
        return c

    tmix[...] = jnp.zeros(tmix.shape, tmix.dtype)
    lax.fori_loop(0, TURNS, temporal, 0)

    loads[4].wait()
    half = rows // TURNS

    def last(turn, c):
        at = pl.ds(pl.multiple_of(turn * half, half), half)
        remote(orecv.at[turn], orecv.at[turn], o_send, o_recv.at[turn], opposite).wait_recv()
        parts = [
            orecv[turn, :, n * piece : (n + 1) * piece, :].reshape(half, LANES)
            for n in range(full)
        ]
        tail = orecv[turn, :, full * piece :, :].astype(F32)
        low = pltpu.roll(tail.reshape(half // 2, LANES), LANES // 2, 1)
        tail = jnp.concatenate([tail, low.reshape(tail.shape)], axis=1)
        parts.append(tail.reshape(half, LANES).astype(BF16))
        out[at, :] = after[at, :] + gate_t * dot(jnp.concatenate(parts, axis=1), two[...])
        return c

    lax.fori_loop(0, TURNS, last, 0)
    remote(stale, kvb.at[2], kv_send.at[0], kv_recv.at[0], opposite).wait_send()
    remote(stale, kvb.at[1], kv_send.at[1], part_recv, partner).wait_send()
    remote(kvb.at[2], kvb.at[3], kv_send.at[2], fwd_recv.at[0], partner).wait_send()
    remote(xs, xs, x_send, x_recv.at[0], opposite).wait_send()
    remote(osend, osend, o_send, o_recv.at[0], opposite).wait_send()


def per_device(
    tokens, stale_kv, mod_table, mod_mix, timestep, frame_order,
    spatial_qkv, spatial_out, temporal_qkv, temporal_out,
):
    rows, width = tokens.shape
    win = spatial_out.shape[0]
    heads = win // (width // HEADS)
    frames = lax.axis_size("patch") // 4
    piece = rows // frames // TURNS
    padded = -(-win // LANES) * LANES
    block = frames * piece
    any_spec = pl.BlockSpec(memory_space=pl.ANY)
    pieces = len(KV_ROWS) - 1
    dma = pltpu.SemaphoreType.DMA
    return pl.pallas_call(
        kernel,
        out_shape=pltpu.VMEM((rows, width), F32),
        in_specs=[any_spec] * 2 + [pl.BlockSpec(memory_space=pltpu.HBM)] * 5 + [any_spec] * 4,
        out_specs=pl.BlockSpec(memory_space=pltpu.VMEM),
        scratch_shapes=[
            pltpu.VMEM(mod_table.shape, F32),
            pltpu.VMEM(mod_table.shape, F32),
            pltpu.SMEM(timestep.shape, jnp.int32),
            pltpu.SMEM(frame_order.shape, jnp.int32),
            pltpu.VMEM((1, width), F32),
            pltpu.VMEM(mod_table.shape, F32),
            pltpu.VMEM((rows, width), BF16),
            pltpu.VMEM((4, rows, width), BF16),
            pltpu.VMEM((3, win, width), BF16),
            pltpu.VMEM((padded, width), BF16),
            pltpu.VMEM((3, win, width), BF16),
            pltpu.VMEM((padded, width), BF16),
            pltpu.VMEM((rows, width), BF16),
            pltpu.VMEM((rows, padded), BF16),
            pltpu.VMEM((heads, rows, WINDOW), BF16),
            pltpu.VMEM((heads, rows, LANES), F32),
            pltpu.VMEM((heads, rows, LANES), F32),
            pltpu.VMEM((heads, rows, WINDOW), F32),
            pltpu.VMEM((rows, padded), BF16),
            pltpu.VMEM((rows, width), F32),
            pltpu.VMEM((rows, width), BF16),
            pltpu.VMEM((TURNS, frames, piece, width), BF16),
            pltpu.VMEM((block, padded), BF16),
            pltpu.VMEM((block, padded), BF16),
            pltpu.VMEM((block, padded), BF16),
            pltpu.VMEM((block, padded), BF16),
            pltpu.VMEM((TURNS, frames, piece * win // LANES, LANES), BF16),
            pltpu.VMEM((TURNS, frames, piece * win // LANES, LANES), BF16),
            dma((5,)), dma((5,)), dma((3,)), dma((pieces,)), dma, dma((pieces,)),
            dma, dma((TURNS,)), dma, dma((TURNS,)),
            pltpu.SemaphoreType.REGULAR((max(frames.bit_length() - 2, 1),)),
        ],
        compiler_params=pltpu.CompilerParams(
            collective_id=0, has_side_effects=True, vmem_limit_bytes=52 * 1024 * 1024
        ),
        name="block",
    )(
        tokens, stale_kv, mod_table, mod_mix, timestep, frame_order,
        jnp.asarray(angular_rates(width)), jnp.swapaxes(spatial_qkv, 1, 2), spatial_out,
        jnp.swapaxes(temporal_qkv, 1, 2), temporal_out,
    )


def solution(mesh):
    return jax.shard_map(
        per_device,
        mesh=mesh,
        in_specs=(
            P(("groups", "patch"), None), P(("groups", "patch"), None), P(), P(),
            P("groups"), P("groups"), P(), P(), P(), P(),
        ),
        out_specs=P(("groups", "patch"), None),
        check_vma=False,
    )
```

```python
import functools
import math

import jax
import jax.numpy as jnp
import numpy as np
from jax import lax
from jax.experimental import pallas as pl
from jax.experimental.pallas import tpu as pltpu
from jax.sharding import PartitionSpec as P

HEADS = 16
EPS = 1e-06
MESH = pl.DeviceIdType.MESH
F32 = jnp.float32
BF16 = jnp.bfloat16
LANES = 128
WINDOW = 256
UNROLL = 8
TURNS = 2
KV_ROWS = (0, 256, 384, 512)
NEG = -1e30


def angular_rates(feature_width):
    half_width = feature_width // 2
    rates = np.exp(-math.log(10000.0) * np.arange(half_width, dtype=np.float64) / half_width)
    return np.concatenate([rates, rates]).astype(np.float32)[None, :]


def sinusoid(position, rates):
    width = rates.shape[1]
    upper = lax.broadcasted_iota(jnp.int32, (1, width), 1) >= width // 2
    angle = position.astype(F32) * rates
    turn = jnp.floor(angle * (2.0 / math.pi) + 0.5)
    x = angle - turn * 1.5703125
    x = x - turn * 4.837512969970703125e-4
    x = x - turn * 7.54978995489188216e-8
    z = x * x
    sine = ((-1.9515295891e-4 * z + 8.3321608736e-3) * z - 1.6666654611e-1) * z * x + x
    cosine = (2.443315711809948e-5 * z - 1.388731625493765e-3) * z + 4.166664568298827e-2
    cosine = cosine * z * z - 0.5 * z + 1.0
    quarter = turn + jnp.where(upper, 1.0, 0.0)
    quarter = quarter - 4.0 * jnp.floor(quarter * 0.25)
    odd = (quarter == 1.0) | (quarter == 3.0)
    value = jnp.where(odd, cosine, sine)
    return jnp.where(quarter >= 2.0, -value, value)


def normalize(v):
    inverse = 1.0 / v.shape[-1]
    mean = jnp.sum(v, axis=-1, keepdims=True) * inverse
    centered = v - mean
    variance = jnp.sum(centered * centered, axis=-1, keepdims=True) * inverse
    return centered * lax.rsqrt(variance + EPS)


def dot(a, b):
    return jnp.dot(a, b, preferred_element_type=F32)


def dot_t(a, b):
    return lax.dot_general(a, b, (((1,), (1,)), ((), ())), preferred_element_type=F32)


def window_start(column, most):
    return pl.multiple_of(jnp.minimum(column // LANES, most) * LANES, LANES)


def wide(x, width):
    return jnp.concatenate([x] * (width // LANES), axis=1) if width > LANES else x


def kernel(
    tokens, stale, table_in, mix_in, time_in, order_in, rates_in, wqkv, wout, tqkv, tout, out,
    table, mix, time, order, rates, mods,
    tok, kvb, wq, wo, tw, two, xin, qb, qm, mx, sm, acc, mixed, after, xs, xr,
    tq, tk, tv, tmix, osend, orecv,
    small_sem, load_sem, kv_send, kv_recv, part_recv, fwd_recv, x_send, x_recv, o_send, o_recv, known,
):
    rows, width = tok.shape
    win = wout.shape[0]
    head_dim = width // HEADS
    heads = win // head_dim
    devices = lax.axis_size("patch")
    frames = devices // 4
    piece = rows // frames // TURNS
    chunk = rows // (2 * TURNS)
    scale = head_dim ** (-0.5) * math.log2(math.e)
    me = lax.axis_index("patch")
    frame, quarter = me // 4, me % 4
    partner = frame * 4 + quarter + 1 - 2 * (quarter % 2)
    across = quarter + 2 - 4 * (quarter // 2)
    opposite = frame * 4 + across
    kv_most = width // LANES - WINDOW // LANES
    q_most = qb.shape[1] // LANES - WINDOW // LANES
    v_tile0 = win // LANES
    pad = win - v_tile0 * LANES

    def remote(src, dst, send, recv, device):
        return pltpu.make_async_remote_copy(
            src_ref=src, dst_ref=dst, send_sem=send, recv_sem=recv,
            device_id={"patch": device}, device_id_type=MESH,
        )

    barrier = pltpu.get_barrier_semaphore()
    chips, chip, core = devices // 2, me // 2, me % 2
    before, after_me = (chip + chips - 1) % chips, (chip + 1) % chips
    near = [partner, before * 2 + core, after_me * 2 + core]
    for device in near:
        pl.semaphore_signal(barrier, inc=1, device_id={"patch": device}, device_id_type=MESH)

    loads = [
        (tokens, tok), (wqkv, wq), (wout, wo.at[pl.ds(pad, win), :]), (tqkv, tw), (tout, two.at[pl.ds(0, win), :]),
    ]
    small = [
        (table_in, table), (mix_in, mix), (time_in, time), (order_in, order), (rates_in, rates),
    ]
    small = [pltpu.make_async_copy(a, b, small_sem.at[i]) for i, (a, b) in enumerate(small)]
    loads = [pltpu.make_async_copy(a, b, load_sem.at[i]) for i, (a, b) in enumerate(loads)]
    for copy in loads[:1] + small:
        copy.start()
    pl.semaphore_wait(barrier, len(near))

    distances = [1 << n for n in range(chips.bit_length() - 2)]

    def say(n):
        for away in (distances[n], chips - distances[n]):
            there = (chip + away) % chips * 2 + core
            pl.semaphore_signal(
                known.at[n], inc=1, device_id={"patch": there}, device_id_type=MESH
            )

    def hear(n):
        pl.semaphore_wait(known.at[n], 2)

    kv_pieces = list(zip(KV_ROWS[:-1], KV_ROWS[1:]))
    for n, (lo, hi) in enumerate(kv_pieces):
        part = stale.at[pl.ds(lo, hi - lo), :]
        remote(part, kvb.at[2, pl.ds(lo, hi - lo), :], kv_send.at[0], kv_recv.at[n], opposite).start()
    remote(stale, kvb.at[1], kv_send.at[1], part_recv, partner).start()
    for copy in loads[1:]:
        copy.start()

    say(0)

    wo[pl.ds(0, pad), :] = jnp.zeros((pad, width), BF16)
    two[pl.ds(win, two.shape[0] - win), :] = jnp.zeros((two.shape[0] - win, width), BF16)
    for ref in (qb, tq, tk, tv):
        ref[...] = jnp.zeros(ref.shape, ref.dtype)
    mixed[...] = jnp.zeros(mixed.shape, mixed.dtype)

    for copy in small:
        copy.wait()
    mods[...] = table[...] + mix[...] * sinusoid(time[0], rates[...])
    position = sinusoid(order[frame], rates[...])
    shift_s, scale_s, gate_s = mods[0:1, :], 1.0 + mods[1:2, :], mods[2:3, :]
    shift_t, scale_t, gate_t = mods[3:4, :] + position, 1.0 + mods[4:5, :], mods[5:6, :]

    loads[0].wait()

    def fresh_in(i, c):
        at = pl.ds(pl.multiple_of(i * chunk, chunk), chunk)
        v = normalize(tok[at, :].astype(F32))
        xin[at, :] = (v * scale_s + shift_s).astype(BF16)
        return c

    lax.fori_loop(0, rows // chunk, fresh_in, 0)
    hear(0)
    say(1)
    loads[1].wait()

    def fresh(i, c):
        at = pl.ds(pl.multiple_of(i * WINDOW, WINDOW), WINDOW)
        x = xin[at, :]
        qb[at, 0:win] = dot_t(x, wq[0]).astype(BF16)
        kvb[0, at, 0:win] = dot_t(x, wq[1]).astype(BF16)
        kvb[0, at, win : 2 * win] = dot_t(x, wq[2]).astype(BF16)
        return c

    lax.fori_loop(0, rows // WINDOW, fresh, 0)
    hear(1)
    say(2)

    whole = pl.ds(0, rows)

    def of_head(start, column, count):
        lane = lax.broadcasted_iota(jnp.int32, (count, WINDOW), 1) + start
        return (lane >= column) & (lane < column + head_dim)

    def each_head(step):
        lax.fori_loop(0, heads, lambda h, c: (step(h), c)[1], 0, unroll=UNROLL)

    def mask_q(h, c):
        start = window_start(h * head_dim, q_most)
        q = qb[:, pl.ds(start, WINDOW)]
        qm[h] = jnp.where(of_head(start, h * head_dim, rows), q, jnp.zeros_like(q))
        mx[h] = jnp.full((rows, LANES), NEG, F32)
        sm[h] = jnp.zeros((rows, LANES), F32)
        acc[h] = jnp.zeros((rows, WINDOW), F32)
        return c

    lax.fori_loop(0, heads, mask_q, 0)

    def attend(h, blocks, own=whole):
        k_at = window_start(h * head_dim, q_most)
        v_at = window_start(win + h * head_dim, kv_most)
        q = qm[h, own, :]
        scores = [dot_t(q, kvb[s, at, pl.ds(k_at, WINDOW)]) for s, at in blocks]
        top = jnp.max(scores[0], axis=-1, keepdims=True)
        for s in scores[1:]:
            top = jnp.maximum(top, jnp.max(s, axis=-1, keepdims=True))
        old = mx[h, own, :]
        new = jnp.maximum(old, top)
        mx[h, own, :] = new
        fade = jnp.exp2((old - new) * scale)
        total = 0.0
        product = 0.0
        for (s, at), score in zip(blocks, scores):
            e = jnp.exp2((score - wide(new, score.shape[1])) * scale)
            total = total + jnp.sum(e, axis=-1, keepdims=True)
            product = product + dot(e.astype(BF16), kvb[s, at, pl.ds(v_at, WINDOW)])
        sm[h, own, :] = sm[h, own, :] * fade + total
        acc[h, own, :] = acc[h, own, :] * wide(fade, WINDOW) + product

    each_head(lambda h: attend(h, [(0, whole)]))
    for n in range(2, len(distances) - 1):
        hear(n)
        say(n + 1)
    remote(stale, kvb.at[1], kv_send.at[1], part_recv, partner).wait_recv()
    each_head(lambda h: attend(h, [(1, whole)]))

    for n, (lo, hi) in enumerate(kv_pieces):
        at = pl.ds(lo, hi - lo)
        remote(stale.at[at, :], kvb.at[2, at, :], kv_send.at[0], kv_recv.at[n], opposite).wait_recv()
        forward = remote(
            kvb.at[2, at, :], kvb.at[3, at, :], kv_send.at[2], fwd_recv.at[n], partner
        )
        forward.start()
        forward.wait_recv()
        if hi < rows:
            each_head(lambda h: attend(h, [(2, at), (3, at)]))

    loads[2].wait()

    for n in range(max(len(distances) - 1, 0), len(distances)):
        hear(n)
    final = pl.ds(kv_pieces[-1][0], rows - kv_pieces[-1][0])

    def finish(u, c):
        at = pl.ds(pl.multiple_of(u * chunk, chunk), chunk)
        each_head(lambda h: attend(h, [(2, final), (3, final)], at))

        def place(h):
            v_at = window_start(win + h * head_dim, kv_most)
            m_at = pl.ds(pl.multiple_of(v_at - v_tile0 * LANES, LANES), WINDOW)
            value = (acc[h, at, :] / wide(sm[h, at, :], WINDOW)).astype(BF16)
            keep = of_head(v_at, win + h * head_dim, chunk)
            mixed[at, m_at] = jnp.where(keep, value, mixed[at, m_at])

        each_head(place)
        done = tok[at, :].astype(F32) + gate_s * dot(mixed[at, :], wo[...])
        after[at, :] = done
        xs[at, :] = (normalize(done) * scale_t + shift_t).astype(BF16)
        turn = u // 2
        for i in (3, 4, 2, 5, 1, 6, 0, 7):
            m = 2 * i + (u + frame) % 2
            j = (frame + m) % frames
            src = pl.ds(pl.multiple_of(u * chunk + (j // 2) * piece, piece), piece)
            remote(
                xs.at[src, :], xr.at[turn, frame], x_send, x_recv.at[turn], j * 4 + across
            ).start()
        return c

    lax.fori_loop(0, 2 * TURNS, finish, 0)

    loads[3].wait()
    full = win // LANES
    block = frames * piece
    same = (
        lax.broadcasted_iota(jnp.int32, (block, block), 0) % piece
        == lax.broadcasted_iota(jnp.int32, (block, block), 1) % piece
    )

    def temporal(turn, c):
        remote(xr.at[turn], xr.at[turn], x_send, x_recv.at[turn], opposite).wait_recv()
        x = xr[turn].reshape(block, width)
        tq[:, 0:win] = dot_t(x, tw[0]).astype(BF16)
        tk[:, 0:win] = dot_t(x, tw[1]).astype(BF16)
        tv[:, 0:win] = dot_t(x, tw[2]).astype(BF16)

        def one_head(h):
            start = window_start(h * head_dim, q_most)
            at = pl.ds(start, WINDOW)
            keep = of_head(start, h * head_dim, block)
            q = tq[:, at]
            score = dot_t(jnp.where(keep, q, jnp.zeros_like(q)), tk[:, at])
            score = jnp.where(same, score, NEG)
            top = jnp.max(score, axis=-1, keepdims=True)
            e = jnp.where(same, jnp.exp2((score - top) * scale), 0.0)
            weights = (e / jnp.sum(e, axis=-1, keepdims=True)).astype(BF16)
            value = dot(weights, tv[:, at]).astype(BF16)
            tmix[:, at] = jnp.where(keep, value, tmix[:, at])

        each_head(one_head)
        for n in range(full):
            part = tmix[:, n * LANES : (n + 1) * LANES]
            osend[turn, :, n * piece : (n + 1) * piece, :] = part.reshape(frames, piece, LANES)
        tail = tmix[:, full * LANES : (full + 1) * LANES].astype(F32)
        tail = tail.reshape(frames, 2, piece // 2, LANES)
        tail = tail[:, 0] + pltpu.roll(tail[:, 1].reshape(block // 2, LANES), LANES // 2, 1).reshape(
            frames, piece // 2, LANES
        )
        osend[turn, :, full * piece :, :] = tail.astype(BF16)
        slot = (frame % 2) * (frames // 2) + frame // 2
        for i in (7, 8, 6, 9, 5, 10, 4, 11, 3, 12, 2, 13, 1, 14, 0, 15):
            j = (frame + i) % frames
            remote(
                osend.at[turn, j], orecv.at[turn, slot], o_send, o_recv.at[turn],
                j * 4 + across,
            ).start()
        return c

    tmix[...] = jnp.zeros(tmix.shape, tmix.dtype)
    lax.fori_loop(0, TURNS, temporal, 0)

    loads[4].wait()
    half = rows // TURNS

    def last(turn, c):
        at = pl.ds(pl.multiple_of(turn * half, half), half)
        remote(orecv.at[turn], orecv.at[turn], o_send, o_recv.at[turn], opposite).wait_recv()
        parts = [
            orecv[turn, :, n * piece : (n + 1) * piece, :].reshape(half, LANES)
            for n in range(full)
        ]
        tail = orecv[turn, :, full * piece :, :].astype(F32)
        low = pltpu.roll(tail.reshape(half // 2, LANES), LANES // 2, 1)
        tail = jnp.concatenate([tail, low.reshape(tail.shape)], axis=1)
        parts.append(tail.reshape(half, LANES).astype(BF16))
        out[at, :] = after[at, :] + gate_t * dot(jnp.concatenate(parts, axis=1), two[...])
        return c

    lax.fori_loop(0, TURNS, last, 0)
    remote(stale, kvb.at[2], kv_send.at[0], kv_recv.at[0], opposite).wait_send()
    remote(stale, kvb.at[1], kv_send.at[1], part_recv, partner).wait_send()
    remote(kvb.at[2], kvb.at[3], kv_send.at[2], fwd_recv.at[0], partner).wait_send()
    remote(xs, xs, x_send, x_recv.at[0], opposite).wait_send()
    remote(osend, osend, o_send, o_recv.at[0], opposite).wait_send()


def per_device(
    tokens, stale_kv, mod_table, mod_mix, timestep, frame_order,
    spatial_qkv, spatial_out, temporal_qkv, temporal_out,
):
    rows, width = tokens.shape
    win = spatial_out.shape[0]
    heads = win // (width // HEADS)
    frames = lax.axis_size("patch") // 4
    piece = rows // frames // TURNS
    padded = -(-win // LANES) * LANES
    block = frames * piece
    any_spec = pl.BlockSpec(memory_space=pl.ANY)
    pieces = len(KV_ROWS) - 1
    dma = pltpu.SemaphoreType.DMA
    return pl.pallas_call(
        kernel,
        out_shape=pltpu.VMEM((rows, width), F32),
        in_specs=[any_spec] * 2 + [pl.BlockSpec(memory_space=pltpu.HBM)] * 5 + [any_spec] * 4,
        out_specs=pl.BlockSpec(memory_space=pltpu.VMEM),
        scratch_shapes=[
            pltpu.VMEM(mod_table.shape, F32),
            pltpu.VMEM(mod_table.shape, F32),
            pltpu.SMEM(timestep.shape, jnp.int32),
            pltpu.SMEM(frame_order.shape, jnp.int32),
            pltpu.VMEM((1, width), F32),
            pltpu.VMEM(mod_table.shape, F32),
            pltpu.VMEM((rows, width), BF16),
            pltpu.VMEM((4, rows, width), BF16),
            pltpu.VMEM((3, win, width), BF16),
            pltpu.VMEM((padded, width), BF16),
            pltpu.VMEM((3, win, width), BF16),
            pltpu.VMEM((padded, width), BF16),
            pltpu.VMEM((rows, width), BF16),
            pltpu.VMEM((rows, padded), BF16),
            pltpu.VMEM((heads, rows, WINDOW), BF16),
            pltpu.VMEM((heads, rows, LANES), F32),
            pltpu.VMEM((heads, rows, LANES), F32),
            pltpu.VMEM((heads, rows, WINDOW), F32),
            pltpu.VMEM((rows, padded), BF16),
            pltpu.VMEM((rows, width), F32),
            pltpu.VMEM((rows, width), BF16),
            pltpu.VMEM((TURNS, frames, piece, width), BF16),
            pltpu.VMEM((block, padded), BF16),
            pltpu.VMEM((block, padded), BF16),
            pltpu.VMEM((block, padded), BF16),
            pltpu.VMEM((block, padded), BF16),
            pltpu.VMEM((TURNS, frames, piece * win // LANES, LANES), BF16),
            pltpu.VMEM((TURNS, frames, piece * win // LANES, LANES), BF16),
            dma((5,)), dma((5,)), dma((3,)), dma((pieces,)), dma, dma((pieces,)),
            dma, dma((TURNS,)), dma, dma((TURNS,)),
            pltpu.SemaphoreType.REGULAR(((2 * frames).bit_length() - 2,)),
        ],
        compiler_params=pltpu.CompilerParams(
            collective_id=0, has_side_effects=True, vmem_limit_bytes=52 * 1024 * 1024
        ),
        name="block",
    )(
        tokens, stale_kv, mod_table, mod_mix, timestep, frame_order,
        jnp.asarray(angular_rates(width)), jnp.swapaxes(spatial_qkv, 1, 2), spatial_out,
        jnp.swapaxes(temporal_qkv, 1, 2), temporal_out,
    )


def solution(mesh):
    return jax.shard_map(
        per_device,
        mesh=mesh,
        in_specs=(
            P(("groups", "patch"), None), P(("groups", "patch"), None), P(), P(),
            P("groups"), P("groups"), P(), P(), P(), P(),
        ),
        out_specs=P(("groups", "patch"), None),
        check_vma=False,
    )
```
